256 devices in a mesh: rep: 4 (over x), fsdp: 32 (over z_lo, y, core), tp: 2 (over z_hi).
Axes of the slice: x: 4, y: 4, z: 8 (z_hi: 2, z_lo: 4; z = z_hi * 4 + z_lo), core: 2. Of those that a mesh axis runs over, the one named last changes fastest.
Arguments:
- hidden: bfloat16 [32768, 4096], P(('rep', 'fsdp')), may hold values from -24 to 24
- norm_gain: float32 [4096], P('fsdp'), may hold values from 0.5 to 1.5
- value_weight: bfloat16 [4096, 1024], P('fsdp', 'tp'), may hold values from -0.09375 to 0.09375
- value_grad: bfloat16 [32768, 1024], P(('rep', 'fsdp'), 'tp'), may hold values from -6 to 6
Outputs:
- input_grad: bfloat16 [32768, 4096], P(('rep', 'fsdp'))
- weight_grad: float32 [4096, 1024], P('fsdp', 'tp')
- gain_grad: float32 [4096], P('fsdp')
The draws below stay inside these ranges and needn't reach their ends.
All inputs are finite; a program needn't handle non-finite values.
Results may differ from the reference program's by a relative error of at most 0.00125.
Values may be sent and summed in bfloat16 or wider, within the bound.
A program may use at most 64 MiB of HBM per device.

```python
import jax
import jax.numpy as jnp
from jax import lax

D = 4096
KV = 1024
TOKENS = 32768
N_REP = 4
N_FSDP = 32


def raised(result, stream_key, source, target, parts, factor):
    def block_of(dim):
        return (jnp.arange(result.shape[dim]) // (result.shape[dim] // parts)).reshape((-1,) + (1,) * (result.ndim - 1 - dim))

    first = jax.random.permutation(stream_key, parts)[block_of(target)]
    other_side = (block_of(target) + parts // 2) % parts
    return jnp.where((block_of(source) == first) | (block_of(source) == other_side), factor * result, result)


def level_of(own_key, extent, pieces, smallest, top_value):
    gain = 1.0
    for position, parts in pieces:
        draws = jax.random.uniform(jax.random.fold_in(jax.random.fold_in(own_key, 6), position), (parts,), jnp.float32, smallest / len(pieces), top_value / len(pieces))
        gain = gain * jnp.repeat(jnp.exp(draws), extent[position] // parts).reshape((-1,) + (1,) * (len(extent) - 1 - position))
    return gain


def centred(stream_key, dims, deviation, reach, shards=(), kind=jnp.bfloat16):
    values = deviation * jax.random.normal(stream_key, dims, jnp.float32)
    if shards:
        values = values * level_of(stream_key, dims, shards, -0.22, 0.18)
    return jnp.clip(values, -reach, reach).astype(kind)


def gaussian_with(stream_key, shape, spread, limit, split, heavy, kind=jnp.bfloat16):
    values = spread * jax.random.normal(stream_key, shape, jnp.float32)
    if split:
        values = values * level_of(stream_key, shape, split, -0.22, 0.18)
    return jnp.clip(raised(values, jax.random.fold_in(stream_key, 3), *heavy), -limit, limit).astype(kind)


def setup_inputs(seed: int = 0) -> dict:
    key_list = jax.random.split(jax.random.key(seed), 5)
    return {
        "hidden": gaussian_with(key_list[0], (TOKENS, D), 1.0, 24.0, ((0, 128),), (0, 1, 128, 5.5)),
        "norm_gain": jnp.clip(1.0 + 0.1 * jax.random.normal(key_list[1], (D,), jnp.float32), 0.5, 1.5),
        "value_weight": centred(key_list[2], (D, KV), D ** -0.5, 0.09375, ((0, 32), (1, 2))),
        "value_grad": centred(key_list[3], (TOKENS, KV), 1.0, 6.0, ((0, 128), (1, 2))),
    }


epsilon = 1e-05

def reference(hidden, norm_gain, value_weight, value_grad):
    inputs = hidden.astype(jnp.float32)
    inv_rms = lax.rsqrt(lax.optimization_barrier(jnp.mean(inputs * inputs, axis=1, keepdims=True)) + epsilon)
    normal = inputs * inv_rms
    normed = (normal * norm_gain).astype(jnp.bfloat16)
    grad_normed = jnp.dot(value_grad, value_weight.T, preferred_element_type=jnp.float32)
    average = 1.0 / (N_REP * N_FSDP)
    weight_grad = jnp.dot(normed.T, value_grad, preferred_element_type=jnp.float32) * average
    gain_grad = lax.optimization_barrier(jnp.sum(grad_normed * normal, axis=0)) * average
    grad_scaled = grad_normed * norm_gain
    center = lax.optimization_barrier(jnp.mean(grad_scaled * normal, axis=1, keepdims=True))
    input_grad = (inv_rms * (grad_scaled - normal * center)).astype(jnp.bfloat16)
    return (input_grad, weight_grad, gain_grad)
```

```python
import jax
import jax.numpy as jnp
from jax import lax
from jax.experimental import pallas as pl
from jax.experimental.pallas import tpu as pltpu
from jax.sharding import PartitionSpec as P

EPS = 1e-05
D = 4096
F32 = jnp.float32
BF16 = jnp.bfloat16
MESH = pl.DeviceIdType.MESH


def kernel(hidden, gain_in, weight_in, grad_in, out_x, out_w, out_g, s):
    rep, fs, tp = lax.axis_index("rep"), lax.axis_index("fsdp"), lax.axis_index("tp")
    X, C, Y = rep, fs % 2, (fs // 2) % 4
    zl, zh = fs // 8, tp
    Z = zh * 4 + zl
    average = 1.0 / 128.0

    def dev(x, y, z, c):
        x, y, z, c = x % 4, y % 4, z % 8, c % 2
        return (x, ((z % 4) * 4 + y) * 2 + c, z // 4)

    def zpeer(k):
        return zh * 4 + (zl + k) % 4

    sibling = dev(X, Y, Z, C + 1)
    started = []

    def send(src, dst, sems, index, target):
        copy = pltpu.make_async_remote_copy(
            src_ref=src,
            dst_ref=dst,
            send_sem=s["sent"].at[len(started)],
            recv_sem=sems.at[index],
            device_id=target,
            device_id_type=MESH,
        )
        copy.start()
        started.append(copy)

    def arrived(dst, sems, index):
        pltpu.make_async_remote_copy(
            src_ref=dst,
            dst_ref=dst,
            send_sem=s["sent"].at[0],
            recv_sem=sems.at[index],
            device_id=sibling,
            device_id_type=MESH,
        ).wait_recv()

    me = X * 2 + C
    wbuf, vgx, vga, hid, hx = s["wbuf"], s["vgx"], s["vga"], s["hid"], s["hx"]
    gainb, invt, invx = s["gainb"], s["invt"], s["invx"]

    w_own = pltpu.make_async_copy(weight_in, wbuf.at[C, Z, Y], s["l_w"])
    w_own.start()
    vg_own = pltpu.make_async_copy(grad_in, vgx.at[me], s["l_vg"].at[0])
    vg_own.start()
    vg_own2 = pltpu.make_async_copy(grad_in, vga.at[zh], s["l_vg"].at[1])
    vg_own2.start()
    loads = []
    for b in range(32):
        load = pltpu.make_async_copy(hidden.at[:, b * 128 : (b + 1) * 128], hid.at[b], s["l_h"].at[b])
        load.start()
        loads.append(load)
    gainb[C, zl, Y] = jnp.broadcast_to(gain_in[...], (8, 128))

    barrier = pltpu.get_barrier_semaphore()

    def greet(target):
        pl.semaphore_signal(barrier, inc=1, device_id=target, device_id_type=MESH)

    for k in range(1, 4):
        for c in range(2):
            greet(dev(X + k, Y, Z, c))
        greet(dev(X, Y + k, Z, C))
        greet(dev(X, Y, zpeer(k), C))
        greet(dev(Y, Y + k, Z, C))
    greet(sibling)
    greet(dev(X, Y, Z + 1, C))
    greet(dev(X, Y, Z - 1, C))
    greet(dev(X, Y, Z + 4, C))

    @pl.when(X != Y)
    def _():
        greet(dev(Y, Y, Z, C))

    pl.semaphore_wait(barrier, 19 + jnp.where(X != Y, 1, 0))

    w_own.wait()

    def w_a(c, z):
        return wbuf.at[c, z, :, 0]

    def w_b(c, z):
        return wbuf.at[c, z, :, 1]

    def w_b1(z, y):
        return wbuf.at[C, z, y, 1]

    for k in (1, 3, 2):
        send(wbuf.at[C, Z, Y, 0], wbuf.at[C, Z, Y, 0], s["a_y"], k, dev(X, Y + k, Z, C))
    send(w_b1(Z, Y), w_b1(Z, Y), s["b_p"], 1, dev(X, Y, Z + 1, C))
    send(w_b1(Z, Y), w_b1(Z, Y), s["b_m"], 1, dev(X, Y, Z - 1, C))
    for k in (1, 3, 2):
        send(gainb.at[C, zl, Y], gainb.at[C, zl, Y], s["g_y"], k, dev(X, Y + k, Z, C))
    vg_own.wait()
    vg_own2.wait()
    for k in (1, 3, 2):
        send(vgx.at[me], vgx.at[me], s["vg_x"], k, dev(X + k, Y, Z, C))
    send(vgx.at[me], vgx.at[me], s["vg_c"], 0, sibling)
    send(vga.at[zh], vga.at[zh], s["vg_t"], 0, dev(X, Y, Z + 4, C))

    def b_to_y(z):
        for k in (1, 3, 2):
            send(w_b1(z, Y), w_b1(z, Y), s["b_y"], (z, k), dev(X, Y + k, Z, C))

    b_to_y(Z)

    for load in loads:
        load.wait()
    own = []
    for zp in range(4):
        for k in (1, 3, 2):
            x = (X + k) % 4
            for c in range(2):
                send(hid.at[zp * 8 + x * 2 + c], hx.at[zp, me], s["h_x"], (zp, me), dev(X + k, Y, Z, c))
        send(hid.at[zp * 8 + X * 2 + 1 - C], hx.at[zp, me], s["h_x"], (zp, me), sibling)
        copy = pltpu.make_async_copy(hid.at[zp * 8 + me], hx.at[zp, me], s["l_o"].at[zp])
        copy.start()
        own.append(copy)

    def square(b, total):
        value = hid[b].astype(F32)
        return total + value * value

    squares = lax.fori_loop(0, 32, square, jnp.zeros((256, 128), F32))
    inv = lax.rsqrt(jnp.sum(squares, axis=1, keepdims=True) * (1.0 / D) + EPS)
    invb = jnp.broadcast_to(inv, (256, 128))
    s["invb"][...] = invb
    invt[...] = jnp.transpose(invb)[:8]
    for k in (1, 3, 2):
        for c in range(2):
            send(invt, invx.at[me], s["i_x"], me, dev(X + k, Y, Z, c))
    send(invt, invx.at[me], s["i_x"], me, sibling)
    s["invc"][me] = invb

    def a_step(k):
        p, m = (Z - k) % 8, (Z + k) % 8
        if k == 0:
            for j in (1, 3, 2):
                arrived(wbuf.at[C, Z, Y - j + jnp.where(Y < j, 4, 0), 0], s["a_y"], j)
            send(w_a(C, Z), w_a(C, Z), s["a_p"], 1, dev(X, Y, Z + 1, C))
            send(w_a(C, Z), w_a(C, Z), s["a_m"], 1, dev(X, Y, Z - 1, C))
            send(w_a(C, Z), w_a(C, Z), s["d_a"], Z, sibling)
        elif k < 4:
            for z, sems, step, part in ((p, s["a_p"], 1, 0), (m, s["a_m"], -1, 2)):
                arrived(w_a(C, z), sems, k)
                if k < 3:
                    send(w_a(C, z), w_a(C, z), sems, k + 1, dev(X, Y, Z + step, C))
                else:
                    half = wbuf.at[C, z, part : part + 2, 0]
                    send(half, half, sems, 4, dev(X, Y, Z + step, C))
                send(w_a(C, z), w_a(C, z), s["d_a"], z, sibling)
        else:
            arrived(wbuf.at[C, p, 0:2, 0], s["a_p"], 4)
            arrived(wbuf.at[C, p, 2:4, 0], s["a_m"], 4)
            send(w_a(C, p), w_a(C, p), s["d_a"], p, sibling)

    def b_step(k):
        p, m = (Z - k) % 8, (Z + k) % 8
        if k < 4:
            for z, sems, step, part in ((p, s["b_p"], 1, 0), (m, s["b_m"], -1, 32)):
                arrived(w_b1(z, Y), sems, k)
                if k < 3:
                    send(w_b1(z, Y), w_b1(z, Y), sems, k + 1, dev(X, Y, Z + step, C))
                else:
                    half = wbuf.at[C, z, Y, 1, part : part + 32]
                    send(half, half, sems, 4, dev(X, Y, Z + step, C))
                b_to_y(z)
        else:
            arrived(wbuf.at[C, p, Y, 1, 0:32], s["b_p"], 4)
            arrived(wbuf.at[C, p, Y, 1, 32:64], s["b_m"], 4)
            b_to_y(p)

    def b_core(z):
        for j in (1, 3, 2):
            arrived(w_b1(z, (Y - j) % 4), s["b_y"], (z, j))
        send(w_b(C, z), w_b(C, z), s["d_b"], z, sibling)

    a_step(0)
    b_step(1)

    for j in (1, 3, 2):
        arrived(gainb.at[C, zl, (Y - j) % 4], s["g_y"], j)
    for k in range(1, 4):
        send(gainb.at[C, zl], gainb.at[C, zl], s["g_z"], k, dev(X, Y, zpeer(k), C))

    a_step(1)
    b_core(Z)
    b_step(2)
    for j in (1, 3, 2):
        x = ((X - j) % 4) * 2 + C
        arrived(vgx.at[x], s["vg_x"], j)
        send(vgx.at[x], vgx.at[x], s["vg_c"], j, sibling)
    for j in range(1, 4):
        arrived(gainb.at[C, (zl - j) % 4], s["g_z"], j)
    send(gainb.at[C], gainb.at[C], s["g_c"], 0, sibling)

    a_step(2)
    b_core((Z - 1) % 8)
    b_core((Z + 1) % 8)
    b_step(3)

    for k in range(1, 8):
        src = (me + k) % 8
        arrived(invx.at[src], s["i_x"], src)
        row = jnp.broadcast_to(invx[src, 0:1], (128, 256))
        s["invc"][src] = jnp.transpose(row)
    for j in range(4):
        src = ((X - j) % 4) * 2 + 1 - C
        arrived(vgx.at[src], s["vg_c"], j)
    arrived(gainb.at[1 - C], s["g_c"], 0)

    part, yrecv, zrecv, ysum = s["part"], s["yrecv"], s["zrecv"], s["ysum"]

    def weight_chunk(zp):
        own[zp].wait()
        for k in range(1, 8):
            src = (me + k) % 8
            arrived(hx.at[zp, src], s["h_x"], (zp, src))
        gain = gainb[C, zp, X]

        def scale(src, _):
            value = (hx[zp, src].astype(F32) * s["invc"][src]).reshape(32, 8, 128) * gain[None]
            s["normed"][src] = value.reshape(256, 128).astype(BF16)
            return 0

        lax.fori_loop(0, 8, scale, 0)
        product = lax.dot_general(
            s["normed"][...].reshape(2048, 128),
            vgx[...].reshape(2048, 512),
            (((0,), (0,)), ((), ())),
            preferred_element_type=F32,
        )
        part[zp] = product.reshape(4, 32, 512)
        for k in (1, 3, 2):
            send(part.at[zp, (Y + k) % 4], yrecv.at[zp, Y], s["r_y"], (zp, Y), dev(X, Y + k, Z, C))

    gg = s["gg"]

    def input_chunk(zq):
        for h in range(2):
            arrived(w_a(1 - C, zq + 4 * h), s["d_a"], zq + 4 * h)
            arrived(w_b(1 - C, zq + 4 * h), s["d_b"], zq + 4 * h)

        def core(c, _):
            product = None
            for h in range(2):
                term = lax.dot_general(
                    vga[h],
                    wbuf[c, zq + 4 * h].reshape(512, 512),
                    (((1,), (1,)), ((), ())),
                    preferred_element_type=F32,
                )
                product = term if product is None else product + term
            for y in range(4):
                value = product[:, y * 128 : (y + 1) * 128]
                b = zq * 8 + y * 2 + c
                share = value * (hid[b].astype(F32) * s["invb"][...])
                share = share.reshape(32, 8, 128)
                gg[c, y, zq] = jnp.sum(share, axis=0)
                gain = gainb[c, zq, y][None]
                s["center"][...] += (share * gain).reshape(256, 128)
                s["gs"][b] = (value.reshape(32, 8, 128) * gain).reshape(256, 128)
            return 0

        lax.fori_loop(0, 2, core, 0)

    s["center"][...] = jnp.zeros((256, 128), F32)

    weight_chunk(0)
    a_step(3)
    b_core((Z - 2) % 8)
    b_core((Z + 2) % 8)
    b_step(4)
    weight_chunk(1)
    a_step(4)
    arrived(vga.at[1 - zh], s["vg_t"], 0)
    input_chunk((zl + 2) % 4)
    weight_chunk(2)
    b_core((Z - 3) % 8)
    b_core((Z + 3) % 8)
    input_chunk((zl + 1) % 4)
    input_chunk((zl + 3) % 4)
    weight_chunk(3)
    b_core((Z + 4) % 8)

    def y_total(zp):
        total = part[zp, Y]
        for j in range(1, 4):
            src = (Y + j) % 4
            arrived(yrecv.at[zp, src], s["r_y"], (zp, src))
            total = total + yrecv[zp, src]
        ysum[zp] = total

    for zp in range(4):
        y_total(zp)
    for k in range(1, 4):
        send(ysum.at[(zl + k) % 4], zrecv.at[zl], s["r_z"], zl, dev(X, Y, zpeer(k), C))

    input_chunk(zl)

    g1, g2, g3, gr1, gr2, gr3, gr4 = (s[n] for n in ("g1", "g2", "g3", "gr1", "gr2", "gr3", "gr4"))
    send(gg.at[1 - C], gr1, s["q_c"], 0, sibling)

    total = ysum[zl]
    for j in range(1, 4):
        src = (zl + j) % 4
        arrived(zrecv.at[src], s["r_z"], src)
        total = total + zrecv[src]
    s["fin"][...] = total * average
    dlv = s["dlv"]
    for k in range(1, 4):
        send(s["fin"], dlv.at[Y], s["r_d"], Y, dev(X + k, X, Z, C))

    @pl.when(X == Y)
    def _():
        dlv[Y] = s["fin"][...]

    def to_diagonal():
        return pltpu.make_async_remote_copy(
            src_ref=s["fin"],
            dst_ref=dlv.at[Y],
            send_sem=s["r_s"],
            recv_sem=s["r_d"].at[Y],
            device_id=dev(X, X, Z, C),
            device_id_type=MESH,
        )

    @pl.when(X != Y)
    def _():
        to_diagonal().start()

    arrived(gr1, s["q_c"], 0)
    g1[...] = gg[C] + gr1[...]
    for k in (1, 3, 2):
        send(g1.at[(Y + k) % 4], gr2.at[Y], s["q_y"], Y, dev(X, Y + k, Z, C))

    center = jnp.sum(s["center"][...], axis=1, keepdims=True) * (1.0 / D)
    s["center"][...] = jnp.broadcast_to(center, (256, 128)) * s["invb"][...]

    def finish(b):
        normal_center = hid[b].astype(F32) * s["center"][...]
        out_x[:, b * 128 : (b + 1) * 128] = (s["invb"][...] * (s["gs"][b] - normal_center)).astype(BF16)

    for b in range(16):
        finish(b)
    gr2[Y] = g1[Y]
    for j in range(1, 4):
        src = (Y + j) % 4
        arrived(gr2.at[src], s["q_y"], src)
    g2[...] = (gr2[0] + gr2[1]) + (gr2[2] + gr2[3])
    for k in range(1, 4):
        send(g2.at[(zl + k) % 4], gr3.at[zl], s["q_z"], zl, dev(X, Y, zpeer(k), C))
    for b in range(16, 32):
        finish(b)
    gr3[zl] = g2[zl]
    for j in range(1, 4):
        src = (zl + j) % 4
        arrived(gr3.at[src], s["q_z"], src)
    g3[...] = (gr3[0] + gr3[1]) + (gr3[2] + gr3[3])
    for k in (1, 3, 2):
        send(g3, gr4.at[X], s["q_x"], X, dev(X + k, Y, Z, C))
    gr4[X] = g3[...]

    for j in range(1, 4):
        src = (Y + j) % 4
        arrived(dlv.at[src], s["r_d"], src)

    @pl.when(X != Y)
    def _():
        arrived(dlv.at[Y], s["r_d"], Y)

    out_w[...] = dlv[...].reshape(128, 512)

    for j in range(1, 4):
        src = (X + j) % 4
        arrived(gr4.at[src], s["q_x"], src)
    result = (gr4[0] + gr4[1]) + (gr4[2] + gr4[3])
    out_g[...] = jnp.sum(result, axis=0, keepdims=True) * average

    for copy in started:
        copy.wait_send()

    @pl.when(X != Y)
    def _():
        to_diagonal().wait_send()


def scratch():
    def sem(*shape):
        return pltpu.SemaphoreType.DMA(shape)

    vmem = pltpu.VMEM
    return dict(
        wbuf=vmem((2, 8, 4, 2, 64, 512), BF16),
        vgx=vmem((8, 256, 512), BF16),
        vga=vmem((2, 256, 512), BF16),
        hid=vmem((32, 256, 128), BF16),
        hx=vmem((4, 8, 256, 128), BF16),
        gainb=vmem((2, 4, 4, 8, 128), F32),
        invt=vmem((8, 256), F32),
        invx=vmem((8, 8, 256), F32),
        invb=vmem((256, 128), F32),
        invc=vmem((8, 256, 128), F32),
        normed=vmem((8, 256, 128), BF16),
        part=vmem((4, 4, 32, 512), F32),
        yrecv=vmem((4, 4, 32, 512), F32),
        ysum=vmem((4, 32, 512), F32),
        zrecv=vmem((4, 32, 512), F32),
        fin=vmem((32, 512), F32),
        dlv=vmem((4, 32, 512), F32),
        gs=vmem((32, 256, 128), F32),
        center=vmem((256, 128), F32),
        gg=vmem((2, 4, 4, 8, 128), F32),
        g1=vmem((4, 4, 8, 128), F32),
        gr1=vmem((4, 4, 8, 128), F32),
        gr2=vmem((4, 4, 8, 128), F32),
        g2=vmem((4, 8, 128), F32),
        gr3=vmem((4, 8, 128), F32),
        g3=vmem((8, 128), F32),
        gr4=vmem((4, 8, 128), F32),
        l_w=pltpu.SemaphoreType.DMA,
        l_vg=pltpu.SemaphoreType.DMA((2,)),
        l_h=pltpu.SemaphoreType.DMA((32,)),
        l_o=pltpu.SemaphoreType.DMA((4,)),
        a_y=sem(4),
        a_p=sem(5),
        a_m=sem(5),
        b_p=sem(5),
        b_m=sem(5),
        b_y=sem(8, 4),
        d_a=sem(8),
        d_b=sem(8),
        g_y=sem(4),
        g_z=sem(4),
        g_c=sem(1),
        vg_x=sem(4),
        vg_c=sem(4),
        vg_t=sem(1),
        h_x=sem(4, 8),
        i_x=sem(8),
        r_y=sem(4, 4),
        r_z=sem(4),
        r_d=sem(4),
        r_s=pltpu.SemaphoreType.DMA,
        sent=sem(176),
        q_c=sem(1),
        q_y=sem(4),
        q_z=sem(4),
        q_x=sem(4),
    )


def local(hidden, norm_gain, value_weight, value_grad):
    any_space = pl.BlockSpec(memory_space=pl.ANY)
    in_vmem = pl.BlockSpec(memory_space=pltpu.VMEM)
    names = scratch()
    input_grad, weight_grad, gain_grad = pl.pallas_call(
        lambda *refs: kernel(*refs[:7], dict(zip(names, refs[7:]))),
        out_shape=(
            jax.ShapeDtypeStruct((256, D), BF16),
            jax.ShapeDtypeStruct((128, 512), F32),
            jax.ShapeDtypeStruct((1, 128), F32),
        ),
        in_specs=[any_space, in_vmem, any_space, any_space],
        out_specs=(in_vmem, in_vmem, in_vmem),
        scratch_shapes=list(names.values()),
        compiler_params=pltpu.CompilerParams(
            collective_id=0, has_side_effects=True, vmem_limit_bytes=48 * 2**20
        ),
        name="rmsnorm_value_backward",
    )(hidden, norm_gain.reshape(1, 128), value_weight.reshape(2, 64, 512), value_grad)
    return (input_grad, weight_grad, gain_grad.reshape(128))


def solution(mesh):
    return jax.shard_map(
        local,
        mesh=mesh,
        in_specs=(P(("rep", "fsdp"), None), P("fsdp"), P("fsdp", "tp"), P(("rep", "fsdp"), "tp")),
        out_specs=(P(("rep", "fsdp"), None), P("fsdp", "tp"), P("fsdp")),
        check_vma=False,
    )
```

```python
import jax
import jax.numpy as jnp
from jax import lax
from jax.experimental import pallas as pl
from jax.experimental.pallas import tpu as pltpu
from jax.sharding import PartitionSpec as P

EPS = 1e-05
SPLIT = 48
MID = 88
SENT = "g_y g_z g_c a_y a_z b_z b_y d vg inv hid r_y r_z r_d q_z q_d r_d_x q_d_x".split()
D = 4096
F32 = jnp.float32
BF16 = jnp.bfloat16
MESH = pl.DeviceIdType.MESH


def kernel(hidden, gain_in, weight_in, grad_in, out_x, out_w, out_g, s):
    rep, fs, tp = lax.axis_index("rep"), lax.axis_index("fsdp"), lax.axis_index("tp")
    X, C, Y = rep, fs % 2, (fs // 2) % 4
    zl, zh = fs // 8, tp
    Z = zh * 4 + zl
    average = 1.0 / 128.0

    def dev(x, y, z, c):
        x, y, z, c = x % 4, y % 4, z % 8, c % 2
        return (x, ((z % 4) * 4 + y) * 2 + c, z // 4)

    def zpeer(k):
        return zh * 4 + (zl + k) % 4

    sibling = dev(X, Y, Z, C + 1)

    def send(src, dst, sent, landed, target):
        copy = pltpu.make_async_remote_copy(
            src_ref=src,
            dst_ref=dst,
            send_sem=s["sent"].at[SENT.index(sent)],
            recv_sem=landed,
            device_id=target,
            device_id_type=MESH,
        )
        copy.start()
        return copy

    def arrived(dst, landed):
        pltpu.make_async_remote_copy(
            src_ref=dst,
            dst_ref=dst,
            send_sem=s["sent"].at[0],
            recv_sem=landed,
            device_id=sibling,
            device_id_type=MESH,
        ).wait_recv()

    def left(sent, src):
        pltpu.make_async_copy(src, src, s["sent"].at[SENT.index(sent)]).wait()

    me = X * 2 + C
    wbuf, vgx, vga, hid, hx = s["wbuf"], s["vgx"], s["vga"], s["hid"], s["hx"]
    gainb, invt, invx = s["gainb"], s["invt"], s["invx"]

    w_own = pltpu.make_async_copy(weight_in, wbuf.at[C, Z, Y], s["l_w"])
    w_own.start()
    gain_own = pltpu.make_async_copy(gain_in, s["gain1"], s["l_g"])
    gain_own.start()
    vg_own = pltpu.make_async_copy(grad_in, vgx.at[me], s["l_vg"].at[0])
    vg_own.start()

    barrier = pltpu.get_barrier_semaphore()

    def greet(target):
        pl.semaphore_signal(barrier, inc=1, device_id=target, device_id_type=MESH)

    for k in range(1, 4):
        for c in range(2):
            greet(dev(X + k, Y, Z, c))
        greet(dev(X, Y + k, Z, C))
        greet(dev(X, Y, zpeer(k), C))
        greet(dev(X, Y, zpeer(k) + 4, C))
        greet(dev(Y, Y + k, Z, C))
    greet(sibling)
    greet(dev(X, Y, Z + 1, C))
    greet(dev(X, Y, Z - 1, C))
    greet(dev(X, Y, Z + 4, C))

    @pl.when(X != Y)
    def _():
        greet(dev(Y, Y, Z, C))

    for b in range(32):
        pltpu.make_async_copy(hidden.at[:, b * 128 : (b + 1) * 128], hid.at[b], s["l_h"]).start()
    vg_own2 = pltpu.make_async_copy(grad_in, vga.at[zh], s["l_vg"].at[1])
    vg_own2.start()
    gain_own.wait()
    gainb[C, zl, Y] = jnp.broadcast_to(s["gain1"][...], (8, 128))
    w_own.wait()
    pl.semaphore_wait(barrier, 22 + jnp.where(X != Y, 1, 0))

    def w_a(c, z):
        return wbuf.at[c, z, :, 0:SPLIT]

    def w_b(c, z):
        return wbuf.at[c, z, :, SPLIT:128]

    def w_b1(z, y, first=SPLIT, last=128):
        return wbuf.at[C, z, y % 4, first:last]

    def b_to_y(z):
        for k, n in ((1, 1), (3, 2)):
            send(w_b1(z, Y), w_b1(z, Y), "b_y", s["b_y"].at[z, n], dev(X, Y + k, Z, C))

    for k in (1, 3, 2):
        send(gainb.at[C, zl, Y], gainb.at[C, zl, Y], "g_y", s["g_y"], dev(X, Y + k, Z, C))
    own_a = wbuf.at[C, Z, Y, 0:SPLIT]
    for k in (1, 3, 2):
        send(own_a, own_a, "a_y", s["a_y"], dev(X, Y + k, Z, C))
    send(w_b1(Z, Y), w_b1(Z, Y), "b_z", s["b_p"].at[0], dev(X, Y, Z + 1, C))
    send(w_b1(Z, Y), w_b1(Z, Y), "b_z", s["b_m"].at[0], dev(X, Y, Z - 1, C))
    vg_own.wait()
    for k, n in ((1, 0), (3, 1)):
        send(vgx.at[me], vgx.at[me], "vg", s["vg_x"].at[n], dev(X + k, Y, Z, C))
    send(vgx.at[me], vgx.at[me], "vg", s["vg_c"], sibling)
    b_to_y(Z)
    vg_own2.wait()

    pltpu.make_async_copy(hid, hid, s["l_h"]).wait()

    def square(b, total):
        value = hid[b].astype(F32)
        return total + value * value

    squares = lax.fori_loop(0, 32, square, jnp.zeros((256, 128), F32))
    inv = lax.rsqrt(jnp.sum(squares, axis=1, keepdims=True) * (1.0 / D) + EPS)
    invb = jnp.broadcast_to(inv, (256, 128))
    s["invb"][...] = invb
    invt[...] = jnp.transpose(invb)[:8]
    s["invc"][me] = invb
    s["center"][...] = jnp.zeros((256, 128), F32)
    for k in (1, 3, 2):
        for c in range(2):
            send(invt, invx.at[me], "inv", s["i_x"], dev(X + k, Y, Z, c))
    send(invt, invx.at[me], "inv", s["i_x"], sibling)

    def hidden_sends(i):
        first = ((zl + 1 + i) % 4) * 8
        for k in (1, 3, 2):
            x = (X + k) % 4
            for c in range(2):
                send(hid.at[first + x * 2 + c], hx.at[i, me], "hid", s["h_x"].at[i], dev(X + k, Y, Z, c))
        send(hid.at[first + X * 2 + 1 - C], hx.at[i, me], "hid", s["h_x"].at[i], sibling)
        pltpu.make_async_copy(hid.at[first + me], hx.at[i, me], s["l_o"]).start()

    hidden_sends(0)

    def values_on():
        first, last = vgx.at[((X - 1) % 4) * 2 + C], vgx.at[((X + 1) % 4) * 2 + C]
        arrived(first, s["vg_x"].at[0])
        send(first.at[0:128], first.at[0:128], "vg", s["vg_x"].at[2], dev(X + 1, Y, Z, C))
        send(first, first, "vg", s["vg_c"], sibling)
        arrived(last, s["vg_x"].at[1])
        send(last.at[128:256], last.at[128:256], "vg", s["vg_x"].at[2], dev(X - 1, Y, Z, C))
        send(last, last, "vg", s["vg_c"], sibling)

    def a_step(k):
        p, m = (Z - k) % 8, (Z + k) % 8
        if k == 0:
            arrived(wbuf.at[C, Z, 0:3, 0:SPLIT], s["a_y"])
            send(w_a(C, Z), w_a(C, Z), "a_z", s["a_p"].at[0], dev(X, Y, Z + 1, C))
            send(w_a(C, Z), w_a(C, Z), "a_z", s["a_m"].at[0], dev(X, Y, Z - 1, C))
            send(w_a(C, Z), w_a(C, Z), "d", s["d"].at[zl], sibling)
        elif k < 4:
            for z, sems, step, part in ((p, s["a_p"], 1, 0), (m, s["a_m"], -1, 2)):
                arrived(w_a(C, z), sems.at[k - 1])
                if k < 3:
                    send(w_a(C, z), w_a(C, z), "a_z", sems.at[k], dev(X, Y, Z + step, C))
                else:
                    half = wbuf.at[C, z, part : part + 2, 0:SPLIT]
                    send(half, half, "a_z", sems.at[3], dev(X, Y, Z + step, C))
                send(w_a(C, z), w_a(C, z), "d", s["d"].at[z % 4], sibling)
        else:
            arrived(wbuf.at[C, p, 0:2, 0:SPLIT], s["a_p"].at[3])
            arrived(wbuf.at[C, p, 2:4, 0:SPLIT], s["a_m"].at[3])
            send(w_a(C, p), w_a(C, p), "d", s["d"].at[p % 4], sibling)

    def b_step(k):
        p, m = (Z - k) % 8, (Z + k) % 8
        if k < 4:
            for z, sems, step, part in ((p, s["b_p"], 1, (SPLIT, MID)), (m, s["b_m"], -1, (MID, 128))):
                arrived(w_b1(z, Y), sems.at[k - 1])
                if k < 3:
                    send(w_b1(z, Y), w_b1(z, Y), "b_z", sems.at[k], dev(X, Y, Z + step, C))
                else:
                    send(w_b1(z, Y, *part), w_b1(z, Y, *part), "b_z", sems.at[3], dev(X, Y, Z + step, C))
                b_to_y(z)
        else:
            arrived(w_b1(p, Y, SPLIT, MID), s["b_p"].at[3])
            arrived(w_b1(p, Y, MID, 128), s["b_m"].at[3])
            b_to_y(p)

    def b_pass(z):
        z = z % 8
        arrived(w_b1(z, Y - 1), s["b_y"].at[z, 1])
        half = w_b1(z, Y - 1, SPLIT, MID)
        send(half, half, "b_y", s["b_y"].at[z, 0], dev(X, Y + 1, Z, C))
        arrived(w_b1(z, Y + 1), s["b_y"].at[z, 2])
        half = w_b1(z, Y + 1, MID, 128)
        send(half, half, "b_y", s["b_y"].at[z, 0], dev(X, Y - 1, Z, C))

    def b_core(z):
        z = z % 8
        arrived(w_b1(z, Y - 2), s["b_y"].at[z, 0])
        send(w_b(C, z), w_b(C, z), "d", s["d"].at[z % 4], sibling)

    part, yrecv, zrecv, ysum = s["part"], s["yrecv"], s["zrecv"], s["ysum"]
    uhi, ulo, gain_part = s["uhi"], s["ulo"], s["gain_part"]

    def weight_chunk(i):
        arrived(hx.at[i, 0:7], s["h_x"].at[i])
        gain = gainb[C, (zl + 1 + i) % 4, X]

        def scale(src, _):
            value = (hx[i, src].astype(F32) * s["invc"][src]).reshape(32, 8, 128) * gain[None]
            s["normed"][src] = value.reshape(256, 128).astype(BF16)
            return 0

        lax.fori_loop(0, 8, scale, 0)
        rows = (((0,), (0,)), ((), ()))
        product = lax.dot_general(
            s["normed"][...].reshape(2048, 128),
            vgx[...].reshape(2048, 512),
            rows,
            preferred_element_type=F32,
        )
        part[i] = product.reshape(4, 32, 512)
        for k in (1, 3, 2):
            send(part.at[i, (Y + k) % 4], yrecv.at[i, Y], "r_y", s["r_y"].at[i], dev(X, Y + k, Z, C))
        raw = hx[i].reshape(2048, 128)
        gain_part[i] = lax.dot_general(
            raw, uhi[...].reshape(2048, 512), rows, preferred_element_type=F32
        ) + lax.dot_general(raw, ulo[...].reshape(2048, 512), rows, preferred_element_type=F32)

    def y_total(i):
        arrived(yrecv.at[i, 0:3], s["r_y"].at[i])
        total = part[i, Y]
        for j in range(1, 4):
            total = total + yrecv[i, (Y + j) % 4]
        if i < 3:
            ysum[i] = total
            send(ysum.at[i], zrecv.at[i], "r_z", s["r_z"], dev(X, Y, zpeer(1 + i), C))
        return total

    def input_chunk(zq):
        zq = zq % 4
        arrived(wbuf.at[1 - C, 0:2], s["d"].at[zq])

        def core(c, _):
            product = None
            for h in range(2):
                term = lax.dot_general(
                    vga[h],
                    wbuf[c, zq + 4 * h].reshape(512, 512),
                    (((1,), (1,)), ((), ())),
                    preferred_element_type=F32,
                )
                product = term if product is None else product + term
            for y in range(4):
                b = zq * 8 + y * 2 + c
                gain = gainb[c, zq, y][None]
                scaled = (product[:, y * 128 : (y + 1) * 128].reshape(32, 8, 128) * gain).reshape(256, 128)
                s["center"][...] += scaled * (hid[b].astype(F32) * s["invb"][...])
                s["gs"][b] = scaled
            return 0

        lax.fori_loop(0, 2, core, 0)

    arrived(gainb.at[C, zl, 0:3], s["g_y"])
    for k in range(1, 4):
        send(gainb.at[C, zl], gainb.at[C, zl], "g_z", s["g_z"], dev(X, Y, zpeer(k), C))
    b_step(1)
    a_step(0)
    b_pass(Z)
    b_step(2)
    b_pass(Z - 1)
    b_pass(Z + 1)
    values_on()
    for i in range(1, 4):
        hidden_sends(i)
    a_step(1)
    arrived(gainb.at[C, 0:3], s["g_z"])
    send(gainb.at[C], gainb.at[C], "g_c", s["g_c"], sibling)
    b_step(3)
    send(vga.at[zh], vga.at[zh], "vg", s["vg_t"], dev(X, Y, Z + 4, C))
    b_core(Z)
    b_pass(Z - 2)
    b_pass(Z + 2)
    arrived(invx.at[0:7], s["i_x"])
    for k in range(1, 8):
        src = (me + k) % 8
        row = jnp.broadcast_to(invx[src, 0:1], (128, 256))
        s["invc"][src] = jnp.transpose(row)
    far = vgx.at[((X + 2) % 4) * 2 + C]
    arrived(far, s["vg_x"].at[2])
    send(far, far, "vg", s["vg_c"], sibling)
    a_step(2)
    arrived(vgx.at[0:4], s["vg_c"])
    arrived(gainb.at[1 - C], s["g_c"])
    pltpu.make_async_copy(hx.at[:, 0], hx.at[:, 0], s["l_o"]).wait()

    def factor(src, _):
        for n in range(4):
            value = vgx[src, :, n * 128 : (n + 1) * 128].astype(F32) * s["invc"][src]
            high = value.astype(BF16)
            uhi[src, :, n * 128 : (n + 1) * 128] = high
            ulo[src, :, n * 128 : (n + 1) * 128] = (value - high.astype(F32)).astype(BF16)
        return 0

    lax.fori_loop(0, 8, factor, 0)
    weight_chunk(0)
    b_step(4)
    b_core(Z - 1)
    b_core(Z + 1)
    b_pass(Z - 3)
    b_pass(Z + 3)
    weight_chunk(1)
    b_core(Z - 2)
    b_core(Z + 2)
    b_pass(Z + 4)
    y_total(0)
    weight_chunk(2)
    a_step(3)
    b_core(Z - 3)
    b_core(Z + 3)
    y_total(1)
    arrived(vga.at[1 - zh], s["vg_t"])
    input_chunk(zl + 2)
    weight_chunk(3)
    b_core(Z + 4)
    a_step(4)
    y_total(2)
    input_chunk(zl + 1)

    q, qr, qd = s["q"], s["qr"], s["qd"]
    for i in range(4):
        z = zh * 4 + (zl + 1 + i) % 4
        terms = gain_part[i] * wbuf[C, z, X].astype(F32)
        column = jnp.sum(terms, axis=1, keepdims=True)
        q[i] = jnp.transpose(jnp.broadcast_to(column, (128, 128)))[:8]
    for i in range(4):
        for h in range(2):
            if i == 3 and h == 0:
                continue
            send(q.at[i], qr.at[Z], "q_z", s["q_z"], dev(X, Y, zpeer(1 + i) + 4 * h, C))
    qr[Z] = q[3]

    input_chunk(zl + 3)
    total = y_total(3)
    arrived(zrecv, s["r_z"])
    for i in range(3):
        total = total + zrecv[i]
    fin, dlv = s["fin"], s["dlv"]
    fin[...] = total * average

    def deliver(src, dst, sent, landed):
        for k in range(1, 4):
            send(src, dst.at[Y], sent, landed, dev(X + k, X, Z, C))

        @pl.when(X == Y)
        def _():
            dst[Y] = src[...]

        def diagonal():
            return pltpu.make_async_remote_copy(
                src_ref=src,
                dst_ref=dst.at[Y],
                send_sem=s["sent"].at[SENT.index(sent + "_x")],
                recv_sem=landed,
                device_id=dev(X, X, Z, C),
                device_id_type=MESH,
            )

        @pl.when(X != Y)
        def _():
            diagonal().start()

        return diagonal

    def delivered(dst, landed):
        @pl.when(X == Y)
        def _():
            arrived(dst.at[0:3], landed)

        @pl.when(X != Y)
        def _():
            arrived(dst, landed)

    late = [deliver(fin, dlv, "r_d", s["r_d"])]
    input_chunk(zl)
    arrived(qr.at[0:7], s["q_z"])
    s["qsum"][...] = ((qr[0] + qr[1]) + (qr[2] + qr[3])) + ((qr[4] + qr[5]) + (qr[6] + qr[7]))
    late.append(deliver(s["qsum"], qd, "q_d", s["q_d"]))

    center = jnp.sum(s["center"][...], axis=1, keepdims=True) * (1.0 / D)
    s["center"][...] = jnp.broadcast_to(center, (256, 128)) * s["invb"][...]
    for b in range(32):
        normal_center = hid[b].astype(F32) * s["center"][...]
        out_x[:, b * 128 : (b + 1) * 128] = (s["invb"][...] * (s["gs"][b] - normal_center)).astype(BF16)

    delivered(dlv, s["r_d"])
    out_w[...] = dlv[...].reshape(128, 512)
    delivered(qd, s["q_d"])
    out_g[...] = ((qd[0] + qd[1]) + (qd[2] + qd[3]))[0:1] * average

    left("g_y", gainb.at[0, 0, 0:3])
    left("g_z", gainb.at[0, 0:3])
    left("g_c", gainb.at[0])
    left("a_y", wbuf.at[0, 0, 0:3, 0:SPLIT])
    left("a_z", wbuf.at[0, 0:7, :, 0:SPLIT])
    left("b_z", wbuf.at[0, 0:7, 0, SPLIT:128])
    left("b_y", wbuf.at[0, 0:6, :, SPLIT:128])
    left("d", wbuf.at[0])
    left("vg", vgx)
    left("inv", invx.at[0:7])
    left("hid", hx.at[:, 0:7])
    left("r_y", yrecv.at[:, 0:3])
    left("r_z", zrecv)
    left("r_d", dlv.at[0:3])
    left("q_z", qr.at[0:7])
    left("q_d", qd.at[0:3])

    @pl.when(X != Y)
    def _():
        for diagonal in late:
            diagonal().wait_send()


def scratch():
    dma = pltpu.SemaphoreType.DMA
    vmem = pltpu.VMEM
    return dict(
        wbuf=vmem((2, 8, 4, 128, 512), BF16),
        vgx=vmem((8, 256, 512), BF16),
        vga=vmem((2, 256, 512), BF16),
        hid=vmem((32, 256, 128), BF16),
        hx=vmem((4, 8, 256, 128), BF16),
        gain1=vmem((1, 128), F32),
        gainb=vmem((2, 4, 4, 8, 128), F32),
        invt=vmem((8, 256), F32),
        invx=vmem((8, 8, 256), F32),
        invb=vmem((256, 128), F32),
        invc=vmem((8, 256, 128), F32),
        normed=vmem((8, 256, 128), BF16),
        part=vmem((4, 4, 32, 512), F32),
        yrecv=vmem((4, 4, 32, 512), F32),
        ysum=vmem((3, 32, 512), F32),
        zrecv=vmem((3, 32, 512), F32),
        fin=vmem((32, 512), F32),
        dlv=vmem((4, 32, 512), F32),
        uhi=vmem((8, 256, 512), BF16),
        ulo=vmem((8, 256, 512), BF16),
        gain_part=vmem((4, 128, 512), F32),
        q=vmem((4, 8, 128), F32),
        qr=vmem((8, 8, 128), F32),
        qd=vmem((4, 8, 128), F32),
        qsum=vmem((8, 128), F32),
        gs=vmem((32, 256, 128), F32),
        center=vmem((256, 128), F32),
        l_w=dma,
        l_g=dma,
        l_h=dma,
        l_o=dma,
        l_vg=dma((2,)),
        sent=dma((len(SENT),)),
        a_y=dma,
        a_p=dma((4,)),
        a_m=dma((4,)),
        b_p=dma((4,)),
        b_m=dma((4,)),
        b_y=dma((8, 3)),
        d=dma((4,)),
        g_y=dma,
        g_z=dma,
        g_c=dma,
        vg_x=dma((3,)),
        vg_c=dma,
        vg_t=dma,
        h_x=dma((4,)),
        i_x=dma,
        r_y=dma((4,)),
        r_z=dma,
        r_d=dma,
        q_z=dma,
        q_d=dma,
    )


def store(*refs):
    copies = [pltpu.make_async_copy(refs[n], refs[n + 3], refs[6].at[n]) for n in range(3)]
    for copy in copies:
        copy.start()
    for copy in copies:
        copy.wait()


def local(hidden, norm_gain, value_weight, value_grad):
    in_hbm = pl.BlockSpec(memory_space=pltpu.HBM)
    in_vmem = pl.BlockSpec(memory_space=pltpu.VMEM)
    names = scratch()
    arrays = (hidden, norm_gain.reshape(1, 128), value_weight, value_grad)
    input_grad, weight_grad, gain_grad = pl.pallas_call(
        lambda *refs: kernel(*refs[:7], dict(zip(names, refs[7:]))),
        out_shape=(
            pltpu.VMEM((256, D), BF16),
            pltpu.VMEM((128, 512), F32),
            pltpu.VMEM((1, 128), F32),
        ),
        in_specs=[in_hbm, in_hbm, in_hbm, in_hbm],
        out_specs=(in_vmem, in_vmem, in_vmem),
        scratch_shapes=list(names.values()),
        compiler_params=pltpu.CompilerParams(
            collective_id=0, has_side_effects=True, vmem_limit_bytes=48 * 2**20
        ),
        name="rmsnorm_value_backward",
    )(*(pltpu.with_memory_space_constraint(x, pltpu.HBM) for x in arrays))
    results = (input_grad, weight_grad, gain_grad)
    input_grad, weight_grad, gain_grad = pl.pallas_call(
        store,
        out_shape=tuple(pltpu.HBM(x.shape, x.dtype) for x in results),
        in_specs=[in_vmem] * 3,
        out_specs=(in_hbm,) * 3,
        scratch_shapes=[pltpu.SemaphoreType.DMA((3,))],
        name="store",
    )(*(pltpu.with_memory_space_constraint(x, pltpu.VMEM) for x in results))
    return (input_grad, weight_grad, gain_grad.reshape(128))


def solution(mesh):
    return jax.shard_map(
        local,
        mesh=mesh,
        in_specs=(P(("rep", "fsdp"), None), P("fsdp"), P("fsdp", "tp"), P(("rep", "fsdp"), "tp")),
        out_specs=(P(("rep", "fsdp"), None), P("fsdp", "tp"), P("fsdp")),
        check_vma=False,
    )
```
